32 devices in a mesh: col: 4 (over y, x), row: 8 (over z, core).
Axes of the slice: x: 2, y: 2, z: 4, core: 2. Of those that a mesh axis runs over, the one named last changes fastest.
Arguments:
- object_field: float32 [2, 4096, 2048], P(None, 'row', 'col'), may hold values from -20 to 20
- probe_field: float32 [2, 256, 256], replicated, may hold values from -4.2 to 4.2
- amplitudes: float32 [8, 4, 2, 256, 256], P('row', 'col'), may hold values from 0.25 to 2.5
- positions: int32 [8, 4, 2, 2], P('row', 'col'), may hold values from -128 to 384, as said below
- batch_order: int32 [8, 4, 2], P('row', 'col'), may hold values from 0 to 1, each once within a row
Outputs:
- object_out: float32 [2, 4096, 2048], P(None, 'row', 'col')
- probe_out: float32 [2, 256, 256], replicated
The draws below stay inside these ranges and needn't reach their ends.
Inputs may be any that keep to these rules, and one draw needn't show every extreme that they name: `positions`: in every tile some pattern's window reaches past its upper edge, some past its lower edge, some past its left edge and some past its right edge. `batch_order`: each tile's 2 entries name each of its patterns once.
All inputs are finite; a program needn't handle non-finite values.
Results may differ from the reference program's by a relative error of at most 0.0065.
Values sent between devices are 32-bit elements; how exact they have to be, the bound alone decides.
A program may use at most 128 MiB of HBM per device.

```python
import math
from functools import partial
import jax
import jax.numpy as jnp
from jax import lax

TILE = 512
W = 256
OV = 128
BS = 1
BATCHES = 2
EPOCHS = 1
PAT = 2
TROWS = 8
TCOLS = 4
NR = 4096
NC = 2048


def draw_object_field(key, part):
    noise_key, rough_key = jax.random.split(key, 2)
    row_frac = jnp.arange(NR, dtype=jnp.float32) / NR
    col_frac = jnp.arange(NC, dtype=jnp.float32) / NC
    trend = jnp.exp(0.5 * math.log(3.0) * (row_frac[:, None] + col_frac[None, :]))
    rough = jax.random.uniform(rough_key, (NR, NC), jnp.float32, 0.5, 1.5)
    base = jnp.clip(jax.random.normal(noise_key, (2, NR, NC), jnp.float32), -6.0, 6.0)
    return 0.7 * base * trend * rough


def draw_positions(key, part):
    depth_key, flip_key, free_key = jax.random.split(jax.random.fold_in(key, 7), 3)
    depth = jax.random.randint(depth_key, (TROWS, TCOLS, 2, PAT), 1, OV + 1, jnp.int32)
    flip = jax.random.randint(flip_key, (TROWS, TCOLS, 2, 1), 0, 2, jnp.int32)
    free = jax.random.randint(free_key, (TROWS, TCOLS, 2, PAT), 0 - OV, TILE - W + OV + 1, jnp.int32)
    index = jnp.arange(PAT, dtype=jnp.int32)[None, None, None, :]
    side = (index + flip) % 2
    edge = jnp.where(side == 0, 0 - depth, TILE - W + depth)
    return jnp.where(index < 2, edge, free).astype(jnp.int32)


def level_of(own_key, dims, shards, smallest, top_value):
    factor_of, own = 1.0, jax.random.fold_in(own_key, 6)
    for position, parts in shards:
        heights = jnp.exp(jax.random.uniform(jax.random.fold_in(own, position), (parts,), jnp.float32, smallest / len(shards), top_value / len(shards)))
        factor_of = factor_of * jnp.repeat(heights, dims[position] // parts).reshape([-1 if axis == position else 1 for axis in range(len(dims))])
    return factor_of


def gaussian(rng, extent, spread, reach, kind=jnp.bfloat16):
    entries = jax.random.normal(rng, extent, jnp.float32) * spread
    return jnp.minimum(jnp.maximum(entries, -reach), reach).astype(kind)


def setup_inputs(seed: int = 0) -> dict:
    streams_of = jax.random.split(jax.random.key(seed), 6)
    object_field = draw_object_field(jax.random.fold_in(streams_of[5], 71), 0)
    probe_field = gaussian(streams_of[1], (2, W, W), 0.7, 4.2, jnp.float32)
    amplitudes = jnp.clip(jnp.exp(math.log(2.5) - 2.3025851 * jax.random.uniform(streams_of[2], (TROWS, TCOLS, PAT, W, W), jnp.float32) ** level_of(streams_of[2], (TROWS, TCOLS, PAT, W, W), ((0, 8), (1, 4)), -0.2, 0.2)), 0.25, 2.5)
    positions = draw_positions(jax.random.fold_in(streams_of[5], 71), 0)
    batch_order = jax.vmap(lambda own: jax.random.permutation(own, PAT))(jax.random.split(streams_of[4], TROWS * TCOLS)).reshape((TROWS, TCOLS, PAT)).astype(jnp.int32)
    return dict(object_field=object_field, probe_field=probe_field, amplitudes=amplitudes, positions=positions, batch_order=batch_order)


ALPHA = 0.5
BETA = 4.0
FLOOR = 0.5
EPSILON = 1e-6


def to_tiles(field):
    return field.reshape(2, TROWS, TILE, TCOLS, TILE).transpose(0, 1, 3, 2, 4)


def from_tiles(tiled):
    return tiled.transpose(0, 1, 3, 2, 4).reshape(2, TROWS * TILE, TCOLS * TILE)


def extend(tiled):
    left_part = jnp.roll(tiled, 1, axis=2)[..., TILE - OV:]
    right_part = jnp.roll(tiled, -1, axis=2)[..., :OV]
    widened = jnp.concatenate([left_part, tiled, right_part], axis=-1)
    upper_part = jnp.roll(widened, 1, axis=1)[..., TILE - OV:, :]
    lower_part = jnp.roll(widened, -1, axis=1)[..., :OV, :]
    return jnp.concatenate([upper_part, widened, lower_part], axis=-2)


def fold_columns(grads):
    own_rows = grads[..., OV:OV + TILE]
    own_rows = own_rows.at[..., :OV].add(jnp.roll(grads[..., OV + TILE:], 1, axis=2))
    own_rows = own_rows.at[..., TILE - OV:].add(jnp.roll(grads[..., :OV], -1, axis=2))
    return own_rows


def tile_gradient(probe_now, batch_index, inputs):
    extended, tile_pos, tile_order, tile_amps = inputs
    picked = tile_order[batch_index * BS:(batch_index + 1) * BS]
    row_pos = tile_pos[0][picked] + OV
    col_pos = tile_pos[1][picked] + OV
    amp_rows = tile_amps[picked]
    zero = jnp.zeros((), jnp.int32)
    windows = jnp.stack([lax.dynamic_slice(extended, (zero, row_pos[member], col_pos[member]), (2, W, W)) for member in range(BS)], axis=1)
    win_re = windows[0]
    win_im = windows[1]
    probe_re = probe_now[0]
    probe_im = probe_now[1]
    wave = lax.complex(probe_re * win_re - probe_im * win_im, probe_re * win_im + probe_im * win_re)
    far_field = jnp.fft.fft2(wave, norm="ortho")
    modulus = jnp.abs(far_field)
    resid = far_field - (amp_rows / jnp.maximum(modulus, FLOOR)) * far_field
    back = jnp.fft.ifft2(resid, norm="ortho")
    back_re = jnp.real(back)
    back_im = jnp.imag(back)
    object_terms = jnp.stack([probe_re * back_re + probe_im * back_im, probe_re * back_im - probe_im * back_re])
    probe_terms = jnp.stack([jnp.sum(win_re * back_re + win_im * back_im, axis=0), jnp.sum(win_re * back_im - win_im * back_re, axis=0)])
    gradient = jnp.zeros_like(extended)
    for member in range(BS):
        start = (zero, row_pos[member], col_pos[member])
        current = lax.dynamic_slice(gradient, start, (2, W, W))
        gradient = lax.dynamic_update_slice(gradient, current + object_terms[:, member], start)
    return gradient, probe_terms


def reference(object_field, probe_field, amplitudes, positions, batch_order):
    span_ext = TILE + 2 * OV
    field_now = to_tiles(object_field)
    probe_now = probe_field
    flat_pos = positions.reshape(TROWS * TCOLS, 2, PAT)
    flat_order = batch_order.reshape(TROWS * TCOLS, PAT)
    flat_amps = amplitudes.reshape(TROWS * TCOLS, PAT, W, W)
    for epoch_index in range(EPOCHS):
        power_total = jnp.sum(field_now * field_now)
        step_object = ALPHA / (jnp.mean(probe_now[0] * probe_now[0] + probe_now[1] * probe_now[1]) + EPSILON)
        deferred = jnp.zeros_like(field_now)
        probe_sum = jnp.zeros_like(probe_now)
        for batch_index in range(BATCHES):
            extended = extend(field_now).transpose(1, 2, 0, 3, 4).reshape(TROWS * TCOLS, 2, span_ext, span_ext)
            grads, probe_terms = lax.map(partial(tile_gradient, probe_now, batch_index), (extended, flat_pos, flat_order, flat_amps))
            grads = grads.reshape(TROWS, TCOLS, 2, span_ext, span_ext).transpose(2, 0, 1, 3, 4)
            probe_sum = probe_sum + jnp.sum(probe_terms, axis=0)
            immediate = fold_columns(grads[..., OV:OV + TILE, :])
            upper_band = fold_columns(grads[..., :OV, :])
            lower_band = fold_columns(grads[..., OV + TILE:, :])
            deferred = deferred.at[..., TILE - OV:, :].add(jnp.roll(upper_band, -1, axis=1))
            deferred = deferred.at[..., :OV, :].add(jnp.roll(lower_band, 1, axis=1))
            field_now = field_now - step_object * immediate
        field_now = field_now - step_object * deferred
        cell_count = NR * NC
        mean_power = power_total / cell_count + EPSILON
        step_probe = BETA * W * W / (cell_count * mean_power)
        probe_now = probe_now - step_probe * probe_sum
    return from_tiles(field_now), probe_now
```

```python
import functools
import math

import jax
import jax.numpy as jnp
import numpy as np
from jax import lax
from jax.experimental import pallas as pl
from jax.experimental.pallas import tpu as pltpu
from jax.sharding import PartitionSpec as P

OV = 128

ALPHA = 0.5
BETA = 4.0
FLOOR = 0.5
EPSILON = 1e-06


def shift(value, axis, steps):
    count = lax.axis_size(axis)
    pairs = [(source, (source + steps) % count) for source in range(count)]
    return lax.ppermute(value, axis, pairs)


def dft_tables(size_w):
    counter = np.arange(size_w)
    angles = 2.0 * math.pi / size_w * (counter[:, None] * counter[None, :] % size_w)
    both = np.concatenate([np.cos(angles), np.sin(angles)], axis=1) / math.sqrt(size_w)
    both = both.astype(np.float32)
    head = both.astype(jnp.bfloat16)
    rest = (both - head.astype(np.float32)).astype(jnp.bfloat16)
    return head, rest


def halves(value):
    head = value.astype(jnp.bfloat16)
    rest = (value - head.astype(jnp.float32)).astype(jnp.bfloat16)
    return head, rest


def dot(left, right):
    return jnp.dot(left, right, preferred_element_type=jnp.float32)


def left_apply(tab_head, tab_rest, re_part, im_part, sign):
    size = re_part.shape[0]
    head, rest = halves(jnp.concatenate([re_part, im_part], axis=1))
    out = dot(tab_head, head) + dot(tab_head, rest) + dot(tab_rest, head)
    cos_re, cos_im = out[:size, :size], out[:size, size:]
    sin_re, sin_im = out[size:, :size], out[size:, size:]
    return cos_re + sign * sin_im, cos_im - sign * sin_re


def right_apply(re_part, im_part, tab_head, tab_rest, sign):
    size = re_part.shape[0]
    head, rest = halves(jnp.concatenate([re_part, im_part], axis=0))
    out = dot(head, tab_head) + dot(rest, tab_head) + dot(head, tab_rest)
    re_cos, re_sin = out[:size, :size], out[:size, size:]
    im_cos, im_sin = out[size:, :size], out[size:, size:]
    return re_cos + sign * im_sin, im_cos - sign * re_sin


def pattern_kernel(
    scal, region, probe, amps, lh, lr, rh, rr, own, to_left, to_right, outer, terms, placed
):
    size_w = probe.shape[-1]
    span = region.shape[-1]
    row_back, col_back, row_on, col_on = scal[0], scal[1], scal[2], scal[3]
    which, up, left = scal[4], scal[5], scal[6]

    def window(part):
        moved = pltpu.roll(region[part], col_back, 1)[:, :size_w]
        return pltpu.roll(moved, row_back, 0)[:size_w]

    win_re, win_im = window(0), window(1)
    probe_re, probe_im = probe[0], probe[1]
    exit_re = probe_re * win_re - probe_im * win_im
    exit_im = probe_re * win_im + probe_im * win_re
    half_re, half_im = left_apply(lh[...], lr[...], exit_re, exit_im, 1.0)
    far_re, far_im = right_apply(half_re, half_im, rh[...], rr[...], 1.0)
    modulus = jnp.sqrt(far_re * far_re + far_im * far_im)
    scaled = amps[which] / jnp.maximum(modulus, FLOOR)
    half_re, half_im = left_apply(
        lh[...], lr[...], far_re - scaled * far_re, far_im - scaled * far_im, -1.0
    )
    back_re, back_im = right_apply(half_re, half_im, rh[...], rr[...], -1.0)
    terms[0] = win_re * back_re + win_im * back_im
    terms[1] = win_re * back_im - win_im * back_re

    def place(part, value):
        below = jnp.zeros((span - size_w, size_w), jnp.float32)
        tall = pltpu.roll(jnp.concatenate([value, below], axis=0), row_on, 0)
        beside = jnp.zeros((span, span - size_w), jnp.float32)
        placed[part] = pltpu.roll(jnp.concatenate([tall, beside], axis=1), col_on, 1)

    place(0, probe_re * back_re + probe_im * back_im)
    place(1, probe_re * back_im - probe_im * back_re)
    half = span - OV
    row_in = pl.ds(pl.multiple_of(up * OV, OV), half)
    row_out = pl.ds(pl.multiple_of((1 - up) * half, OV), OV)
    col_in = pl.ds(pl.multiple_of(left * OV, OV), half)
    is_left = left == 1
    zero = jnp.zeros((), jnp.float32)
    for part in range(2):
        own[part] = placed[part, row_in, col_in]
        to_left[part] = jnp.where(is_left, placed[part, row_in, :OV], zero)
        to_right[part] = jnp.where(is_left, zero, placed[part, row_in, half:])
        outer[part] = placed[part, row_out, :]


def pattern(scal, region, probe, amps, tables):
    size_w = probe.shape[-1]
    span = region.shape[-1]
    half = span - OV
    head, rest = tables
    vmem = pl.BlockSpec(memory_space=pltpu.VMEM)
    f32 = lambda *shape: jax.ShapeDtypeStruct(shape, jnp.float32)
    flops = 12 * 2 * (2 * size_w) ** 2 * size_w
    return pl.pallas_call(
        pattern_kernel,
        out_shape=(
            f32(2, half, half),
            f32(2, half, OV),
            f32(2, half, OV),
            f32(2, OV, span),
            f32(2, size_w, size_w),
        ),
        in_specs=[pl.BlockSpec(memory_space=pltpu.SMEM)] + [vmem] * 7,
        out_specs=(vmem,) * 5,
        scratch_shapes=[pltpu.VMEM((2, span, span), jnp.float32)],
        compiler_params=pltpu.CompilerParams(vmem_limit_bytes=40 * 1024 * 1024),
        cost_estimate=pl.CostEstimate(
            flops=flops, bytes_accessed=6 * 1024 * 1024, transcendentals=2 * size_w * size_w
        ),
    )(
        scal,
        region,
        probe,
        amps,
        jnp.asarray(np.concatenate(np.split(head, 2, axis=1), axis=0)),
        jnp.asarray(np.concatenate(np.split(rest, 2, axis=1), axis=0)),
        jnp.asarray(head),
        jnp.asarray(rest),
    )


def region_of(field, up, left, up_of_left, up_of_right):
    tile = field.shape[1]
    half = tile // 2
    above = shift(field[:, tile - OV :], "row", 1)
    below = shift(field[:, :OV], "row", -1)

    def tall(start, stop, is_up):
        cols = slice(start, stop)
        upper = jnp.concatenate([above[..., cols], field[:, :half, cols]], axis=1)
        lower = jnp.concatenate([field[:, half:, cols], below[..., cols]], axis=1)
        return jnp.where(is_up, upper, lower)

    right_side = shift(tall(0, OV, up_of_left), "col", -1)
    left_side = shift(tall(tile - OV, tile, up_of_right), "col", 1)
    return jnp.where(
        left,
        jnp.concatenate([left_side, tall(0, half, up)], axis=2),
        jnp.concatenate([tall(half, tile, up), right_side], axis=2),
    )


def rows_at(value, is_up):
    blank = jnp.zeros_like(value)
    return jnp.where(
        is_up,
        jnp.concatenate([value, blank], axis=1),
        jnp.concatenate([blank, value], axis=1),
    )


def cols_at(value, is_left):
    blank = jnp.zeros_like(value)
    return jnp.where(
        is_left,
        jnp.concatenate([value, blank], axis=2),
        jnp.concatenate([blank, value], axis=2),
    )


def sides(from_left, from_right, tile):
    middle = jnp.zeros(from_left.shape[:2] + (tile - 2 * OV,), jnp.float32)
    return jnp.concatenate([from_left, middle, from_right], axis=2)


def local(object_field, probe_field, amplitudes, positions, batch_order):
    size_w = probe_field.shape[-1]
    tile = object_field.shape[1]
    half = tile // 2
    span = half + OV
    tables = dft_tables(size_w)
    cell_count = float(tile * tile * lax.axis_size("col") * lax.axis_size("row"))
    step_object = ALPHA / (
        jnp.mean(probe_field[0] * probe_field[0] + probe_field[1] * probe_field[1]) + EPSILON
    )
    power_local = jnp.sum(object_field * object_field)

    order = batch_order[0, 0]
    row_pos = positions[0, 0, 0][order]
    col_pos = positions[0, 0, 1][order]
    flags = jnp.stack([row_pos[0] < 0, col_pos[0] < 0]).astype(jnp.int32)
    flags_left = shift(flags, "col", 1)
    flags_right = shift(flags, "col", -1)
    flags_above = shift(flags, "row", 1)
    flags_below = shift(flags, "row", -1)

    field = object_field
    outers, probe_sum = [], 0.0
    for batch in range(2):
        turn = lambda flag: (flag == 1) if batch == 0 else (flag == 0)
        up, left = turn(flags[0]), turn(flags[1])
        up_of_left, up_of_right = turn(flags_left[0]), turn(flags_right[0])
        region = region_of(field, up, left, up_of_left, up_of_right)
        row_on = jnp.where(up, row_pos[batch] + OV, row_pos[batch] - half)
        col_on = jnp.where(left, col_pos[batch] + OV, col_pos[batch] - half)
        scal = jnp.stack(
            [
                (span - row_on) % span,
                (span - col_on) % span,
                row_on,
                col_on,
                order[batch],
                up.astype(jnp.int32),
                left.astype(jnp.int32),
            ]
        )
        own, to_left, to_right, outer, terms = pattern(
            scal, region, probe_field, amplitudes[0, 0], tables
        )
        probe_sum = probe_sum + terms
        outers.append(outer)
        came_right = shift(to_left, "col", -1)
        came_left = shift(to_right, "col", 1)
        total = cols_at(rows_at(own, up), left) + sides(
            rows_at(came_left, up_of_left), rows_at(came_right, up_of_right), tile
        )
        if batch == 0:
            field = field - step_object * total

    first_up = flags[0] == 1
    going_up = jnp.where(first_up, outers[0], outers[1])
    going_down = jnp.where(first_up, outers[1], outers[0])
    from_below = shift(going_up, "row", -1)
    from_above = shift(going_down, "row", 1)
    lefts = (flags_above[0] != flags_above[1], flags_below[0] == flags_below[1])
    inner, corner_left, corner_right = [], [], []
    for band, is_left in zip((from_above, from_below), lefts):
        inner.append(cols_at(jnp.where(is_left, band[..., OV:], band[..., :half]), is_left))
        corner_left.append(jnp.where(is_left, band[..., :OV], 0.0))
        corner_right.append(jnp.where(is_left, 0.0, band[..., half:]))
    corner_came_right = shift(jnp.concatenate(corner_left, axis=1), "col", -1)
    corner_came_left = shift(jnp.concatenate(corner_right, axis=1), "col", 1)
    corners = sides(corner_came_left, corner_came_right, tile)
    blank = jnp.zeros((2, tile - 2 * OV, tile), jnp.float32)
    bands = jnp.concatenate(
        [inner[0] + corners[:, :OV], blank, inner[1] + corners[:, OV:]], axis=1
    )
    field = field - step_object * (total + bands)

    packed = jnp.concatenate([probe_sum, jnp.full((2, 8, size_w), power_local)], axis=1)
    packed = lax.psum(packed, ("col", "row"))
    mean_power = packed[0, size_w, 0] / cell_count + EPSILON
    step_probe = BETA * size_w * size_w / (cell_count * mean_power)
    return field, probe_field - step_probe * packed[:, :size_w]


def solution(mesh):
    return jax.shard_map(
        local,
        mesh=mesh,
        in_specs=(
            P(None, "row", "col"),
            P(),
            P("row", "col", None, None, None),
            P("row", "col", None, None),
            P("row", "col", None),
        ),
        out_specs=(P(None, "row", "col"), P()),
        check_vma=False,
    )
```

```python
import functools
import math

import jax
import jax.numpy as jnp
import numpy as np
from jax import lax
from jax.experimental import pallas as pl
from jax.experimental.pallas import tpu as pltpu
from jax.sharding import PartitionSpec as P

OV = 128

ALPHA = 0.5
BETA = 4.0
FLOOR = 0.5
EPSILON = 1e-06


def shift(value, axis, steps):
    count = lax.axis_size(axis)
    pairs = [(source, (source + steps) % count) for source in range(count)]
    return lax.ppermute(value, axis, pairs)


def dft_tables(size_w):
    counter = np.arange(size_w)
    angles = 2.0 * math.pi / size_w * (counter[:, None] * counter[None, :] % size_w)
    both = np.concatenate([np.cos(angles), np.sin(angles)], axis=1) / math.sqrt(size_w)
    both = both.astype(np.float32)
    head = both.astype(jnp.bfloat16)
    rest = (both - head.astype(np.float32)).astype(jnp.bfloat16)
    return head, rest


def halves(value):
    head = value.astype(jnp.bfloat16)
    rest = (value - head.astype(jnp.float32)).astype(jnp.bfloat16)
    return head, rest


def dot(left, right):
    return jnp.dot(left, right, preferred_element_type=jnp.float32)


def left_apply(tab_head, tab_rest, re_part, im_part, sign):
    size = re_part.shape[0]
    head, rest = halves(jnp.concatenate([re_part, im_part], axis=1))
    out = dot(tab_head, head) + dot(tab_head, rest) + dot(tab_rest, head)
    cos_re, cos_im = out[:size, :size], out[:size, size:]
    sin_re, sin_im = out[size:, :size], out[size:, size:]
    return cos_re + sign * sin_im, cos_im - sign * sin_re


def right_apply(re_part, im_part, tab_head, tab_rest, sign):
    size = re_part.shape[0]
    head, rest = halves(jnp.concatenate([re_part, im_part], axis=0))
    out = dot(head, tab_head) + dot(rest, tab_head) + dot(head, tab_rest)
    re_cos, re_sin = out[:size, :size], out[:size, size:]
    im_cos, im_sin = out[size:, :size], out[size:, size:]
    return re_cos + sign * im_sin, im_cos - sign * re_sin


def pattern_kernel(
    scal, region, probe, amps, lh, lr, rh, rr, own, to_left, to_right, outer, terms, placed
):
    size_w = probe.shape[-1]
    span = region.shape[-1]
    row_back, col_back, row_on, col_on = scal[0], scal[1], scal[2], scal[3]
    which, up, left = scal[4], scal[5], scal[6]

    def window(part):
        moved = pltpu.roll(region[part], col_back, 1)[:, :size_w]
        return pltpu.roll(moved, row_back, 0)[:size_w]

    win_re, win_im = window(0), window(1)
    probe_re, probe_im = probe[0], probe[1]
    exit_re = probe_re * win_re - probe_im * win_im
    exit_im = probe_re * win_im + probe_im * win_re
    half_re, half_im = left_apply(lh[...], lr[...], exit_re, exit_im, 1.0)
    far_re, far_im = right_apply(half_re, half_im, rh[...], rr[...], 1.0)
    modulus = jnp.sqrt(far_re * far_re + far_im * far_im)
    scaled = amps[which] / jnp.maximum(modulus, FLOOR)
    half_re, half_im = left_apply(
        lh[...], lr[...], far_re - scaled * far_re, far_im - scaled * far_im, -1.0
    )
    back_re, back_im = right_apply(half_re, half_im, rh[...], rr[...], -1.0)
    terms[0] = win_re * back_re + win_im * back_im
    terms[1] = win_re * back_im - win_im * back_re

    def place(part, value):
        below = jnp.zeros((span - size_w, size_w), jnp.float32)
        tall = pltpu.roll(jnp.concatenate([value, below], axis=0), row_on, 0)
        beside = jnp.zeros((span, span - size_w), jnp.float32)
        placed[part] = pltpu.roll(jnp.concatenate([tall, beside], axis=1), col_on, 1)

    place(0, probe_re * back_re + probe_im * back_im)
    place(1, probe_re * back_im - probe_im * back_re)
    half = span - OV
    row_in = pl.ds(pl.multiple_of(up * OV, OV), half)
    row_out = pl.ds(pl.multiple_of((1 - up) * half, OV), OV)
    col_in = pl.ds(pl.multiple_of(left * OV, OV), half)
    is_left = left == 1
    zero = jnp.zeros((), jnp.float32)
    for part in range(2):
        own[part] = placed[part, row_in, col_in]
        to_left[part] = jnp.where(is_left, placed[part, row_in, :OV], zero)
        to_right[part] = jnp.where(is_left, zero, placed[part, row_in, half:])
        outer[part] = placed[part, row_out, :]


def pattern(scal, region, probe, amps, tables):
    size_w = probe.shape[-1]
    span = region.shape[-1]
    half = span - OV
    head, rest = tables
    vmem = pl.BlockSpec(memory_space=pltpu.VMEM)
    f32 = lambda *shape: jax.ShapeDtypeStruct(shape, jnp.float32)
    flops = 12 * 2 * (2 * size_w) ** 2 * size_w
    return pl.pallas_call(
        pattern_kernel,
        out_shape=(
            f32(2, half, half),
            f32(2, half, OV),
            f32(2, half, OV),
            f32(2, OV, span),
            f32(2, size_w, size_w),
        ),
        in_specs=[pl.BlockSpec(memory_space=pltpu.SMEM)] + [vmem] * 7,
        out_specs=(vmem,) * 5,
        scratch_shapes=[pltpu.VMEM((2, span, span), jnp.float32)],
        compiler_params=pltpu.CompilerParams(vmem_limit_bytes=40 * 1024 * 1024),
        cost_estimate=pl.CostEstimate(
            flops=flops, bytes_accessed=6 * 1024 * 1024, transcendentals=2 * size_w * size_w
        ),
    )(
        scal,
        region,
        probe,
        amps,
        jnp.asarray(np.concatenate(np.split(head, 2, axis=1), axis=0)),
        jnp.asarray(np.concatenate(np.split(rest, 2, axis=1), axis=0)),
        jnp.asarray(head),
        jnp.asarray(rest),
    )


def sum_kernel(
    steps, data, power, out, power_out, acc, got, back, mine, theirs, sends, recvs, psends, precvs
):
    barrier = pltpu.get_barrier_semaphore()
    bits, partners = [], []
    for axis, stride in steps:
        index = lax.axis_index(axis)
        bit = (index // stride) % 2
        bits.append(bit)
        partners.append({axis: index + stride - 2 * stride * bit})
    for partner in partners:
        pl.semaphore_signal(
            barrier, inc=1, device_id=partner, device_id_type=pl.DeviceIdType.MESH
        )
    pl.semaphore_wait(barrier, len(steps))

    def send(source, target, send_sem, recv_sem, step):
        copy = pltpu.make_async_remote_copy(
            src_ref=source,
            dst_ref=target,
            send_sem=send_sem,
            recv_sem=recv_sem,
            device_id=partners[step],
            device_id_type=pl.DeviceIdType.MESH,
        )
        copy.start()
        return copy

    low, count, offset, halved = 0, data.shape[0], 0, []
    held, held_power = data, power
    for step in range(len(steps)):
        halving = count % 2 == 0
        part = count // 2 if halving else count
        keep = low + bits[step] * part if halving else low
        give = low + (1 - bits[step]) * part if halving else low
        landing = pl.ds(offset, part)
        main = send(
            held.at[pl.ds(give, part)], got.at[landing], sends.at[step], recvs.at[step], step
        )
        side = send(held_power, theirs.at[step], psends.at[step], precvs.at[step], step)
        main.wait()
        side.wait()
        acc[pl.ds(keep, part)] = held[pl.ds(keep, part)] + got[landing]
        mine[step] = held_power[...] + theirs[step]
        held, held_power = acc, mine.at[step]
        low, count, offset = keep, part, offset + part
        if halving:
            halved.append(step)
    for place, step in enumerate(reversed(halved)):
        sem = len(steps) + place
        block = pl.ds(low, count)
        send(acc.at[block], back.at[block], sends.at[sem], recvs.at[sem], step).wait()
        other = pl.ds(low + (1 - 2 * bits[step]) * count, count)
        acc[other] = back[other]
        low, count = low - bits[step] * count, 2 * count
    out[...] = acc[...]
    power_out[...] = mine[len(steps) - 1]


def sum_all(data, power, mesh_shape):
    steps = [("row", 1)] if mesh_shape["row"] > 1 else []
    steps += [("col", 2**k) for k in range(mesh_shape["col"].bit_length() - 1)]
    steps += [("row", 2**k) for k in range(1, mesh_shape["row"].bit_length() - 1)]
    number = len(steps)
    vmem = pl.BlockSpec(memory_space=pltpu.VMEM)
    dma = pltpu.SemaphoreType.DMA
    return pl.pallas_call(
        functools.partial(sum_kernel, steps),
        out_shape=(
            jax.ShapeDtypeStruct(data.shape, jnp.float32),
            jax.ShapeDtypeStruct(power.shape, jnp.float32),
        ),
        in_specs=[vmem, vmem],
        out_specs=(vmem, vmem),
        scratch_shapes=[
            pltpu.VMEM(data.shape, jnp.float32),
            pltpu.VMEM((data.shape[0] + number,) + data.shape[1:], jnp.float32),
            pltpu.VMEM(data.shape, jnp.float32),
            pltpu.VMEM((number,) + power.shape, jnp.float32),
            pltpu.VMEM((number,) + power.shape, jnp.float32),
            dma((2 * number,)),
            dma((2 * number,)),
            dma((number,)),
            dma((number,)),
        ],
        compiler_params=pltpu.CompilerParams(
            collective_id=0, has_side_effects=True, vmem_limit_bytes=16 * 1024 * 1024
        ),
        cost_estimate=pl.CostEstimate(flops=0, bytes_accessed=40_000_000, transcendentals=0),
    )(data, power)


def region_of(field, up, left, up_of_left, up_of_right):
    tile = field.shape[1]
    half = tile // 2
    above = shift(field[:, tile - OV :], "row", 1)
    below = shift(field[:, :OV], "row", -1)

    def tall(start, stop, is_up):
        cols = slice(start, stop)
        upper = jnp.concatenate([above[..., cols], field[:, :half, cols]], axis=1)
        lower = jnp.concatenate([field[:, half:, cols], below[..., cols]], axis=1)
        return jnp.where(is_up, upper, lower)

    right_side = shift(tall(0, OV, up_of_left), "col", -1)
    left_side = shift(tall(tile - OV, tile, up_of_right), "col", 1)
    return jnp.where(
        left,
        jnp.concatenate([left_side, tall(0, half, up)], axis=2),
        jnp.concatenate([tall(half, tile, up), right_side], axis=2),
    )


def rows_at(value, is_up):
    blank = jnp.zeros_like(value)
    return jnp.where(
        is_up,
        jnp.concatenate([value, blank], axis=1),
        jnp.concatenate([blank, value], axis=1),
    )


def cols_at(value, is_left):
    blank = jnp.zeros_like(value)
    return jnp.where(
        is_left,
        jnp.concatenate([value, blank], axis=2),
        jnp.concatenate([blank, value], axis=2),
    )


def sides(from_left, from_right, tile):
    middle = jnp.zeros(from_left.shape[:2] + (tile - 2 * OV,), jnp.float32)
    return jnp.concatenate([from_left, middle, from_right], axis=2)


def local(mesh_shape, object_field, probe_field, amplitudes, positions, batch_order):
    size_w = probe_field.shape[-1]
    tile = object_field.shape[1]
    half = tile // 2
    span = half + OV
    tables = dft_tables(size_w)
    cell_count = float(tile * tile * lax.axis_size("col") * lax.axis_size("row"))
    step_object = ALPHA / (
        jnp.mean(probe_field[0] * probe_field[0] + probe_field[1] * probe_field[1]) + EPSILON
    )
    power_local = jnp.sum(object_field * object_field)

    order = batch_order[0, 0]
    row_pos = positions[0, 0, 0][order]
    col_pos = positions[0, 0, 1][order]
    flags = jnp.stack([row_pos[0] < 0, col_pos[0] < 0]).astype(jnp.int32)
    flags_left = shift(flags, "col", 1)
    flags_right = shift(flags, "col", -1)
    flags_above = shift(flags, "row", 1)
    flags_below = shift(flags, "row", -1)

    field = object_field
    outers, probe_sum = [], 0.0
    for batch in range(2):
        turn = lambda flag: (flag == 1) if batch == 0 else (flag == 0)
        up, left = turn(flags[0]), turn(flags[1])
        up_of_left, up_of_right = turn(flags_left[0]), turn(flags_right[0])
        region = region_of(field, up, left, up_of_left, up_of_right)
        row_on = jnp.where(up, row_pos[batch] + OV, row_pos[batch] - half)
        col_on = jnp.where(left, col_pos[batch] + OV, col_pos[batch] - half)
        scal = jnp.stack(
            [
                (span - row_on) % span,
                (span - col_on) % span,
                row_on,
                col_on,
                order[batch],
                up.astype(jnp.int32),
                left.astype(jnp.int32),
            ]
        )
        own, to_left, to_right, outer, terms = pattern(
            scal, region, probe_field, amplitudes[0, 0], tables
        )
        probe_sum = probe_sum + terms
        outers.append(outer)
        came_right = shift(to_left, "col", -1)
        came_left = shift(to_right, "col", 1)
        total = cols_at(rows_at(own, up), left) + sides(
            rows_at(came_left, up_of_left), rows_at(came_right, up_of_right), tile
        )
        if batch == 0:
            field = field - step_object * total

    first_up = flags[0] == 1
    going_up = jnp.where(first_up, outers[0], outers[1])
    going_down = jnp.where(first_up, outers[1], outers[0])
    from_below = shift(going_up, "row", -1)
    from_above = shift(going_down, "row", 1)
    lefts = (flags_above[0] != flags_above[1], flags_below[0] == flags_below[1])
    inner, corner_left, corner_right = [], [], []
    for band, is_left in zip((from_above, from_below), lefts):
        inner.append(cols_at(jnp.where(is_left, band[..., OV:], band[..., :half]), is_left))
        corner_left.append(jnp.where(is_left, band[..., :OV], 0.0))
        corner_right.append(jnp.where(is_left, 0.0, band[..., half:]))
    corner_came_right = shift(jnp.concatenate(corner_left, axis=1), "col", -1)
    corner_came_left = shift(jnp.concatenate(corner_right, axis=1), "col", 1)
    corners = sides(corner_came_left, corner_came_right, tile)
    blank = jnp.zeros((2, tile - 2 * OV, tile), jnp.float32)
    bands = jnp.concatenate(
        [inner[0] + corners[:, :OV], blank, inner[1] + corners[:, OV:]], axis=1
    )
    field = field - step_object * (total + bands)

    summed, power_total = sum_all(
        probe_sum.reshape(-1, 8, size_w), jnp.full((8, 128), power_local), mesh_shape
    )
    mean_power = power_total[0, 0] / cell_count + EPSILON
    step_probe = BETA * size_w * size_w / (cell_count * mean_power)
    return field, probe_field - step_probe * summed.reshape(probe_field.shape)


def solution(mesh):
    return jax.shard_map(
        functools.partial(local, dict(mesh.shape)),
        mesh=mesh,
        in_specs=(
            P(None, "row", "col"),
            P(),
            P("row", "col", None, None, None),
            P("row", "col", None, None),
            P("row", "col", None),
        ),
        out_specs=(P(None, "row", "col"), P()),
        check_vma=False,
    )
```
